256 devices in a mesh: gx: 8 (over y, core), gy: 16 (over z, x_lo), gz: 2 (over x_hi).
Axes of the slice: x: 4 (x_hi: 2, x_lo: 2; x = x_hi * 2 + x_lo), y: 4, z: 8, core: 2. Of those that a mesh axis runs over, the one named last changes fastest.
Arguments:
- directions: float32 [8, 128, 256, 256], P(None, 'gx', 'gy', 'gz'), may hold values from -6 to 6
- state: float32 [128, 256, 256], P('gx', 'gy', 'gz'), may hold values from -2 to 2
- log_cond: float32 [128, 256, 256], P('gx', 'gy', 'gz'), may hold values from -1 to 1
- obs_mask: int32 [128, 256, 256], P('gx', 'gy', 'gz'), may hold values 0 or 1
Outputs:
- hessian_action: float32 [8, 128, 256, 256], P(None, 'gx', 'gy', 'gz')
- quotient: float32 [8], replicated
The draws below stay inside these ranges and needn't reach their ends.
All inputs are finite; a program needn't handle non-finite values. No bound on the sum of `obs_mask` on one device may be relied on, other than what follows from the above.
Results may differ from the reference program's by a relative error of at most 0.00002.
Values sent between devices are 32-bit elements; how exact they have to be, the bound alone decides.
A program may use at most 128 MiB of HBM per device.

```python
import math
import jax
import jax.numpy as jnp
from jax import lax

NDIR = 8
ITERS = 4
NX = 128
NY = 256
NZ = 256


def place_ends(entries, key, least, top_value):
    shape = entries.shape
    place = [jax.random.randint(jax.random.fold_in(key, axis), (), 0, shape[axis]) for axis in range(len(shape))]
    entries = entries.at[tuple(place)].set(least)
    longest = shape.index(max(shape))
    place[longest] = (place[longest] + 1) % shape[longest]
    return entries.at[tuple(place)].set(top_value)


def levels(key, shape, split, smallest, high):
    def one(dim, parts):
        steps = jax.random.uniform(jax.random.fold_in(jax.random.fold_in(key, 6), dim), (parts,), jnp.float32, smallest / len(split), high / len(split))
        return jnp.repeat(jnp.exp(steps), shape[dim] // parts).reshape((-1,) + (1,) * (len(shape) - dim - 1))

    level = one(*split[0])
    for cut in split[1:]:
        level = level * one(*cut)
    return level


def normal_values(rng, dims, deviation, limit, split=(), dtype=jnp.bfloat16):
    result = deviation * jax.random.normal(rng, dims, jnp.float32)
    if split:
        result = result * levels(rng, dims, split, -0.22, 0.18)
    return jnp.clip(result, -limit, limit).astype(dtype)


def setup_inputs(seed: int = 0) -> dict:
    seeds = jax.random.split(jax.random.key(seed), 5)
    directions = normal_values(seeds[0], (NDIR, NX, NY, NZ), 1.0, 6.0, ((1, 8), (2, 16), (3, 2)), jnp.float32)
    state = normal_values(seeds[1], (NX, NY, NZ), 0.3, 2.0, ((0, 8), (1, 16), (2, 2)), jnp.float32)
    log_cond = jnp.clip(jax.random.uniform(seeds[2], (NX, NY, NZ), jnp.float32, -1.0, 1.0) * levels(seeds[2], (NX, NY, NZ), ((0, 8), (1, 16), (2, 2)), -0.4, 0.0), -1.0, 1.0)
    obs_mask = place_ends((jax.random.randint(seeds[3], (NX, NY, NZ), 0, 4) < 1).astype(jnp.int32), jax.random.fold_in(seeds[3], 1), 0, 1)
    return {"directions": directions, "state": state, "log_cond": log_cond, "obs_mask": obs_mask}


SHIFT = 0.3
BETA = 0.05
DATA_WEIGHT = 10.0


def chebyshev(count):
    return [1.0 / (1.125 + 0.825 * math.cos(math.pi * (2 * j + 1) / (2 * count))) for j in range(count)]


def neighbours(padded):
    total = padded[..., 2:, 1:-1, 1:-1] + padded[..., :-2, 1:-1, 1:-1]
    total = total + padded[..., 1:-1, 2:, 1:-1] + padded[..., 1:-1, :-2, 1:-1]
    return total + padded[..., 1:-1, 1:-1, 2:] + padded[..., 1:-1, 1:-1, :-2]


def padone(field):
    return jnp.pad(field, 1)


def reference(directions, state, log_cond, obs_mask):
    conduct = jnp.exp(log_cond)
    diagonal = SHIFT + 6.0 * conduct
    lap_state = 6.0 * state - neighbours(padone(state))
    observed = obs_mask.astype(jnp.float32)
    cheb_w = chebyshev(ITERS)

    def single(delta):
        source = -conduct * delta * lap_state
        tangent = cheb_w[0] * source / diagonal
        for step in range(1, ITERS):
            applied = diagonal * tangent - conduct * neighbours(padone(tangent))
            tangent = tangent + cheb_w[step] * (source - applied) / diagonal
        data_rhs = DATA_WEIGHT * observed * tangent
        adjoint = cheb_w[0] * data_rhs / diagonal
        for step in range(1, ITERS):
            applied = diagonal * adjoint - neighbours(padone(conduct * adjoint))
            adjoint = adjoint + cheb_w[step] * (data_rhs - applied) / diagonal
        hessian = -conduct * lap_state * adjoint + BETA * (6.0 * delta - neighbours(padone(delta)))
        return hessian, jnp.sum(delta * hessian) / (NX * NY * NZ)

    hessian_action, quotient = lax.map(single, directions)
    return hessian_action, quotient
```

```python
import math

import jax
import jax.numpy as jnp
from jax import lax
from jax.experimental import pallas as pl
from jax.experimental.pallas import tpu as pltpu
from jax.sharding import PartitionSpec as P

ITERS = 4
SHIFT = 0.3
BETA = 0.05
DATA_WEIGHT = 10.0

NDIR = 8
EDGE = 16
LANES = 128
DENSE = EDGE * EDGE
PITCH = 24
ROWS = (EDGE + 2) * PITCH
PER = 2
GROUPS = NDIR // PER

DELTA, T1, T2, B0, B1, B2, T0 = range(7)
EXCHANGES = 6
STATE, FIRST = range(2)


def chebyshev(count):
    return [
        1.0 / (1.125 + 0.825 * math.cos(math.pi * (2 * j + 1) / (2 * count))) for j in range(count)
    ]


def dense(x):
    return pl.ds(x * EDGE, EDGE)


def plane(x):
    return pl.ds((x + 1) * PITCH, EDGE)


def row(y):
    return pl.ds(PITCH + y, EDGE, stride=PITCH)


def kernel(
    sizes,
    d_hbm,
    s_hbm,
    c_hbm,
    m_hbm,
    out_hbm,
    quo_ref,
    d_in,
    s_in,
    c_in,
    m_in,
    field,
    y_send,
    y_halo,
    z_send,
    z_halo,
    coef,
    cy_send,
    cy_halo,
    cz_send,
    cz_halo,
    ratio,
    lap,
    weight,
    forcing,
    smooth,
    result,
    partial,
    sum_x,
    sum_y,
    sum_z,
    load_sem,
    dload_sem,
    out_sem,
    send_sem,
    recv_sem,
    csend_sem,
    crecv_sem,
    rsend_sem,
    rrecv_sem,
):
    gx, gy, gz = sizes
    ix, iy, iz = lax.axis_index("gx"), lax.axis_index("gy"), lax.axis_index("gz")
    cheb = chebyshev(ITERS)

    def along_x(o):
        return (lax.rem(ix + o, gx), iy, iz)

    def along_y(o):
        return (ix, lax.rem(iy + o, gy), iz)

    across = (ix, iy, 1 - iz)
    partners = [along_x(o) for o in range(1, gx)] + [along_y(o) for o in range(1, gy)] + [across]

    barrier = pltpu.get_barrier_semaphore()
    for partner in partners:
        pl.semaphore_signal(barrier, inc=1, device_id=partner, device_id_type=pl.DeviceIdType.MESH)

    loads = [
        pltpu.make_async_copy(s_hbm, s_in, load_sem.at[0]),
        pltpu.make_async_copy(c_hbm, c_in, load_sem.at[1]),
        pltpu.make_async_copy(m_hbm, m_in, load_sem.at[2]),
    ]

    def load_group(g):
        dirs = pl.ds(g * PER, PER)
        return pltpu.make_async_copy(d_hbm.at[dirs], d_in.at[dirs], dload_sem.at[g])

    loads[0].start()
    for g in range(GROUPS):
        load_group(g).start()
    loads[1].start()
    loads[2].start()

    targets = [
        (ix - 1, iy, iz),
        (ix + 1, iy, iz),
        (ix, iy - 1, iz),
        (ix, iy + 1, iz),
        across,
    ]
    exists = [ix > 0, ix < gx - 1, iy > 0, iy < gy - 1, None]
    order = (2, 3, 4, 0, 1)

    def where_exists(side):
        return (lambda f: f()) if exists[side] is None else pl.when(exists[side])

    def faces(e, g):
        dirs = pl.ds(g * PER, PER)
        leave = [
            field.at[e, dirs, plane(0)],
            field.at[e, dirs, plane(EDGE - 1)],
            y_send.at[e, 0, dirs],
            y_send.at[e, 1, dirs],
            z_send.at[e, g],
        ]
        arrive = [
            field.at[e, dirs, plane(-1)],
            field.at[e, dirs, plane(EDGE)],
            y_halo.at[e, 0, dirs],
            y_halo.at[e, 1, dirs],
            z_halo.at[e, g],
        ]
        return leave, arrive, send_sem.at[e, g], recv_sem.at[e, g]

    def coef_faces(e):
        leave = [
            coef.at[e, plane(0)],
            coef.at[e, plane(EDGE - 1)],
            cy_send.at[e, 0],
            cy_send.at[e, 1],
            cz_send.at[e],
        ]
        arrive = [
            coef.at[e, plane(-1)],
            coef.at[e, plane(EDGE)],
            cy_halo.at[e, 0],
            cy_halo.at[e, 1],
            cz_halo.at[e],
        ]
        return leave, arrive, csend_sem.at[e], crecv_sem.at[e]

    opposite = (1, 0, 3, 2, 4)

    def outgoing(parts, side):
        leave, arrive, sent, received = parts
        return pltpu.make_async_remote_copy(
            src_ref=leave[side],
            dst_ref=arrive[opposite[side]],
            send_sem=sent.at[side],
            recv_sem=received.at[opposite[side]],
            device_id=targets[side],
            device_id_type=pl.DeviceIdType.MESH,
        )

    def incoming(parts, side):
        leave, arrive, sent, received = parts
        return pltpu.make_async_remote_copy(
            src_ref=leave[side],
            dst_ref=arrive[side],
            send_sem=sent.at[side],
            recv_sem=received.at[side],
            device_id=targets[side],
            device_id_type=pl.DeviceIdType.MESH,
        )

    def send(parts):
        for side in order:

            @where_exists(side)
            def _():
                outgoing(parts, side).start()

    def wait_faces(parts):
        for side in order:

            @where_exists(side)
            def _():
                incoming(parts, side).wait_recv()

    def wait_sent(parts):
        for side in order:

            @where_exists(side)
            def _():
                outgoing(parts, side).wait_send()

    nothing = jnp.zeros((EDGE, LANES), jnp.float32)
    for side in range(4):

        @pl.when(jnp.logical_not(exists[side]))
        def _():
            for e in range(2):
                if side < 2:
                    coef[e, plane(-1 if side == 0 else EDGE), :] = nothing
                else:
                    cy_halo[e, side - 2] = nothing

            @pl.loop(0, EXCHANGES)
            def _(e):
                for dd in range(NDIR):
                    if side < 2:
                        field[e, dd, plane(-1 if side == 0 else EDGE), :] = nothing
                    else:
                        y_halo[e, side - 2, dd] = nothing

    lane = lax.broadcasted_iota(jnp.int32, (EDGE, LANES), 1)
    first_lane, last_lane = lane == 0, lane == LANES - 1
    inner_lane = jnp.where(iz == 0, LANES - 1, 0)
    faces_partner = lane == inner_lane
    lane8 = lax.broadcasted_iota(jnp.int32, (8, LANES), 1)
    slot = lax.rem(lane8 - inner_lane + LANES, LANES)

    def pack(packed, values, place):
        for half in range(2):
            k = place + half
            moved = values[8 * half : 8 * half + 8]
            if k:
                moved = pltpu.roll(moved, k, 1)
            packed = jnp.where(slot == k, moved, packed)
        return packed

    def arrived(packed):
        return jnp.where(iz == 0, pltpu.roll(packed, LANES - 1, 1), pltpu.roll(packed, 1, 1))

    def unpack(packed, place):
        halves = [pltpu.roll(packed, (LANES - place - h) % LANES, 1) for h in range(2)]
        return jnp.concatenate(halves, axis=0)

    def stencil(load, x, packed, place):
        centre = load(0)
        below = jnp.where(first_lane, 0.0, pltpu.roll(centre, 1, 1))
        above = jnp.where(last_lane, 0.0, pltpu.roll(centre, LANES - 1, 1))
        beyond = jnp.where(faces_partner, unpack(packed, place), 0.0)
        total = (load(-PITCH) + load(PITCH)) + (load(-1) + load(1))
        return centre, total + ((below + above) + beyond)

    def field_stencil(e, dd, x, packed, dl):
        def load(offset):
            return field[e, dd, pl.ds((x + 1) * PITCH + offset, EDGE), :]

        return stencil(load, x, packed, dl * 2 * EDGE + 2 * x)

    empty = jnp.zeros((8, LANES), jnp.float32)

    def finish_coef(e, packed):
        cy_send[e, 0] = coef[e, row(0), :]
        cy_send[e, 1] = coef[e, row(EDGE - 1), :]
        cz_send[e] = packed
        send(coef_faces(e))

    def coef_rows(e):
        coef[e, row(-1), :] = cy_halo[e, 0]
        coef[e, row(EDGE), :] = cy_halo[e, 1]

    def finish_dir(e, dd):
        y_send[e, 0, dd] = field[e, dd, row(0), :]
        y_send[e, 1, dd] = field[e, dd, row(EDGE - 1), :]

    def field_rows(e, dd):
        field[e, dd, row(-1), :] = y_halo[e, 0, dd]
        field[e, dd, row(EDGE), :] = y_halo[e, 1, dd]

    loads[0].wait()
    packed = empty
    for x in range(EDGE):
        values = s_in[dense(x), :]
        coef[STATE, plane(x), :] = values
        packed = pack(packed, values, 2 * x)
    pl.semaphore_wait(barrier, len(partners))
    finish_coef(STATE, packed)

    @pl.loop(0, GROUPS)
    def _(g):
        load_group(g).wait()
        packed = empty
        for dl in range(PER):
            dd = g * PER + dl
            for x in range(EDGE):
                values = d_in[dd, dense(x), :]
                field[DELTA, dd, plane(x), :] = values
                packed = pack(packed, values, dl * 2 * EDGE + 2 * x)
            finish_dir(DELTA, dd)
        z_send[DELTA, g] = packed
        send(faces(DELTA, g))

    loads[1].wait()
    for x in range(EDGE):
        conduct = jnp.exp(c_in[dense(x), :])
        ratio[dense(x), :] = conduct / (SHIFT + 6.0 * conduct)
    loads[2].wait()
    for x in range(EDGE):
        weight[dense(x), :] = DATA_WEIGHT * m_in[dense(x), :].astype(jnp.float32)

    wait_faces(coef_faces(STATE))
    coef_rows(STATE)
    state_z = arrived(cz_halo[STATE])
    packed = empty
    for x in range(EDGE):

        def load(offset, x=x):
            return coef[STATE, pl.ds((x + 1) * PITCH + offset, EDGE), :]

        centre, total = stencil(load, x, state_z, 2 * x)
        lap_here = 6.0 * centre - total
        lap[dense(x), :] = lap_here
        first = -cheb[0] * ratio[dense(x), :] * lap_here
        coef[FIRST, plane(x), :] = first
        packed = pack(packed, first, 2 * x)
    finish_coef(FIRST, packed)

    @pl.loop(0, GROUPS)
    def _(g):
        wait_faces(faces(DELTA, g))
        delta_z = arrived(z_halo[DELTA, g])
        for dl in range(PER):
            dd = g * PER + dl
            field_rows(DELTA, dd)
            total = nothing
            for x in range(EDGE):
                centre, near = field_stencil(DELTA, dd, x, delta_z, dl)
                part = BETA * (6.0 * centre - near)
                smooth[dd, dense(x), :] = part
                total = total + centre * part
                forcing[dd, dense(x), :] = -lap[dense(x), :] * centre
                field[T0, dd, plane(x), :] = coef[FIRST, plane(x), :] * centre
            partial[dd] = total[:8] + total[8:]

    def advance(g, src, packed, w, sink):
        carry = empty
        for dl in range(PER):
            dd = g * PER + dl
            carry = sink.begin(dd, carry)
            for x in range(EDGE):
                centre, near = field_stencil(src, dd, x, packed, dl)
                step = ratio[dense(x), :] * (forcing[dd, dense(x), :] + near) - centre
                carry = sink.plane(dd, dl, x, centre + w * step, carry)
            sink.end(dd)
        return carry

    class Iterate:
        def __init__(self, dst):
            self.dst = dst

        def begin(self, dd, carry):
            return carry

        def plane(self, dd, dl, x, values, carry):
            field[self.dst, dd, plane(x), :] = values
            return pack(carry, values, dl * 2 * EDGE + 2 * x)

        def end(self, dd):
            finish_dir(self.dst, dd)

    class Observe(Iterate):
        def begin(self, dd, carry):
            self.total = nothing
            return carry

        def plane(self, dd, dl, x, values, carry):
            rhs = weight[dense(x), :] * values
            forcing[dd, dense(x), :] = rhs
            self.total = self.total + rhs * values
            first = cheb[0] * ratio[dense(x), :] * rhs
            return super().plane(dd, dl, x, first, carry)

        def end(self, dd):
            partial[dd] = partial[dd] + (self.total[:8] + self.total[8:])
            super().end(dd)

    class Result:
        def begin(self, dd, carry):
            return carry

        def plane(self, dd, dl, x, values, carry):
            result[dd, dense(x), :] = smooth[dd, dense(x), :] - lap[dense(x), :] * values
            return carry

        def end(self, dd):
            pass

    def step(src, sink, w):
        @pl.loop(0, GROUPS)
        def _(g):
            wait_faces(faces(src, g))
            for dl in range(PER):
                field_rows(src, g * PER + dl)
            packed = advance(g, src, arrived(z_halo[src, g]), w, sink)
            if isinstance(sink, Iterate):
                z_send[sink.dst, g] = packed
                send(faces(sink.dst, g))
            else:
                store_group(g).start()

    def store_group(g):
        dirs = pl.ds(g * PER, PER)
        return pltpu.make_async_copy(result.at[dirs], out_hbm.at[dirs], out_sem.at[g])

    wait_faces(coef_faces(FIRST))
    first_z = arrived(cz_halo[FIRST])
    repeated = first_z
    for dl in range(1, PER):
        repeated = repeated + pltpu.roll(first_z, dl * 2 * EDGE, 1)

    @pl.loop(0, GROUPS)
    def _(g):
        for dl in range(PER):
            dd = g * PER + dl
            for x in (-1, EDGE):
                field[T0, dd, plane(x), :] = coef[FIRST, plane(x), :] * field[DELTA, dd, plane(x), :]
            field[T0, dd, row(-1), :] = cy_halo[FIRST, 0] * y_halo[DELTA, 0, dd]
            field[T0, dd, row(EDGE), :] = cy_halo[FIRST, 1] * y_halo[DELTA, 1, dd]
        start_z = repeated * arrived(z_halo[DELTA, g])
        z_send[T1, g] = advance(g, T0, start_z, cheb[1], Iterate(T1))
        send(faces(T1, g))

    step(T1, Iterate(T2), cheb[2])
    step(T2, Observe(B0), cheb[3])

    def reduce_start(buf, mine, count, at, base, value):
        buf[mine] = value
        for o in range(1, count):
            pltpu.make_async_remote_copy(
                src_ref=buf.at[mine],
                dst_ref=buf.at[mine],
                send_sem=rsend_sem.at[base + o],
                recv_sem=rrecv_sem.at[base + o],
                device_id=at(o),
                device_id_type=pl.DeviceIdType.MESH,
            ).start()

    def reduce_copy(buf, slot_index, count, at, base, o):
        return pltpu.make_async_remote_copy(
            src_ref=buf.at[slot_index],
            dst_ref=buf.at[slot_index],
            send_sem=rsend_sem.at[base + o],
            recv_sem=rrecv_sem.at[base + o],
            device_id=at(o),
            device_id_type=pl.DeviceIdType.MESH,
        )

    def reduce_end(buf, mine, count, at, base):
        for o in range(1, count):
            reduce_copy(buf, lax.rem(mine + count - o, count), count, at, base, o).wait_recv()
        total = buf[0]
        for i in range(1, count):
            total = total + buf[i]
        return total

    rounds = (
        (sum_x, ix, gx, along_x, 0),
        (sum_y, iy, gy, along_y, gx),
        (sum_z, iz, gz, lambda o: across, gx + gy),
    )

    reduce_start(*rounds[0], jnp.sum(partial[...], axis=1))
    step(B0, Iterate(B1), cheb[1])
    reduce_start(*rounds[1], reduce_end(*rounds[0]))
    step(B1, Iterate(B2), cheb[2])
    reduce_start(*rounds[2], reduce_end(*rounds[1]))
    step(B2, Result(), cheb[3])
    quo_ref[...] = reduce_end(*rounds[2])

    @pl.loop(0, GROUPS)
    def _(g):
        for e in range(EXCHANGES):
            wait_sent(faces(e, g))
        store_group(g).wait()

    for e in range(2):
        wait_sent(coef_faces(e))
    for buf, mine, count, at, base in rounds:
        for o in range(1, count):
            reduce_copy(buf, mine, count, at, base, o).wait_send()


def solution(mesh):
    sizes = tuple(mesh.shape[name] for name in ("gx", "gy", "gz"))
    gx, gy, gz = sizes
    assert gz == 2
    f32 = jnp.float32
    cells = gx * gy * gz * DENSE * LANES

    def shards(directions, state, log_cond, obs_mask):
        assert directions.shape == (NDIR, EDGE, EDGE, LANES)
        any_spec = pl.BlockSpec(memory_space=pl.ANY)
        out, sums = pl.pallas_call(
            lambda *refs: kernel(sizes, *refs),
            out_shape=(
                jax.ShapeDtypeStruct((NDIR, DENSE, LANES), f32),
                jax.ShapeDtypeStruct((NDIR, LANES), f32),
            ),
            in_specs=[any_spec] * 4,
            out_specs=(any_spec, pl.BlockSpec(memory_space=pltpu.VMEM)),
            scratch_shapes=[
                pltpu.VMEM((NDIR, DENSE, LANES), f32),
                pltpu.VMEM((DENSE, LANES), f32),
                pltpu.VMEM((DENSE, LANES), f32),
                pltpu.VMEM((DENSE, LANES), jnp.int32),
                pltpu.VMEM((EXCHANGES + 1, NDIR, ROWS, LANES), f32),
                pltpu.VMEM((EXCHANGES, 2, NDIR, EDGE, LANES), f32),
                pltpu.VMEM((EXCHANGES, 2, NDIR, EDGE, LANES), f32),
                pltpu.VMEM((EXCHANGES, GROUPS, 8, LANES), f32),
                pltpu.VMEM((EXCHANGES, GROUPS, 8, LANES), f32),
                pltpu.VMEM((2, ROWS, LANES), f32),
                pltpu.VMEM((2, 2, EDGE, LANES), f32),
                pltpu.VMEM((2, 2, EDGE, LANES), f32),
                pltpu.VMEM((2, 8, LANES), f32),
                pltpu.VMEM((2, 8, LANES), f32),
                pltpu.VMEM((DENSE, LANES), f32),
                pltpu.VMEM((DENSE, LANES), f32),
                pltpu.VMEM((DENSE, LANES), f32),
                pltpu.VMEM((NDIR, DENSE, LANES), f32),
                pltpu.VMEM((NDIR, DENSE, LANES), f32),
                pltpu.VMEM((NDIR, DENSE, LANES), f32),
                pltpu.VMEM((NDIR, 8, LANES), f32),
                pltpu.VMEM((gx, NDIR, LANES), f32),
                pltpu.VMEM((gy, NDIR, LANES), f32),
                pltpu.VMEM((gz, NDIR, LANES), f32),
                pltpu.SemaphoreType.DMA((3,)),
                pltpu.SemaphoreType.DMA((GROUPS,)),
                pltpu.SemaphoreType.DMA((GROUPS,)),
                pltpu.SemaphoreType.DMA((EXCHANGES, GROUPS, 5)),
                pltpu.SemaphoreType.DMA((EXCHANGES, GROUPS, 5)),
                pltpu.SemaphoreType.DMA((2, 5)),
                pltpu.SemaphoreType.DMA((2, 5)),
                pltpu.SemaphoreType.DMA((gx + gy + gz,)),
                pltpu.SemaphoreType.DMA((gx + gy + gz,)),
            ],
            compiler_params=pltpu.CompilerParams(collective_id=0, has_side_effects=True),
        )(
            directions.reshape(NDIR, DENSE, LANES),
            state.reshape(DENSE, LANES),
            log_cond.reshape(DENSE, LANES),
            obs_mask.reshape(DENSE, LANES),
        )
        return out.reshape(directions.shape), jnp.sum(sums, axis=1) / cells

    placed = P("gx", "gy", "gz")
    stacked = P(None, "gx", "gy", "gz")
    return jax.shard_map(
        shards,
        mesh=mesh,
        in_specs=(stacked, placed, placed, placed),
        out_specs=(stacked, P()),
        check_vma=False,
    )
```

```python
import math

import jax
import jax.numpy as jnp
from jax import lax
from jax.experimental import pallas as pl
from jax.experimental.pallas import tpu as pltpu
from jax.sharding import PartitionSpec as P

ITERS = 4
SHIFT = 0.3
BETA = 0.05
DATA_WEIGHT = 10.0

NDIR = 8
EDGE = 16
LANES = 128
DENSE = EDGE * EDGE
PITCH = 24
ROWS = (EDGE + 2) * PITCH
PER = 2
GROUPS = NDIR // PER

DELTA, T1, T2, B0, B1, B2, T0 = range(7)
EXCHANGES = 6
STATE, FIRST = range(2)
GREETED = (0, 1, 2)


def chebyshev(count):
    return [
        1.0 / (1.125 + 0.825 * math.cos(math.pi * (2 * j + 1) / (2 * count))) for j in range(count)
    ]


def dense(x):
    return pl.ds(x * EDGE, EDGE)


def plane(x):
    return pl.ds((x + 1) * PITCH, EDGE)


def row(y):
    return pl.ds(PITCH + y, EDGE, stride=PITCH)


def kernel(
    sizes,
    d_hbm,
    s_hbm,
    c_hbm,
    m_hbm,
    result,
    quo_ref,
    d_in,
    s_in,
    c_in,
    m_in,
    field,
    y_send,
    y_halo,
    z_send,
    z_halo,
    coef,
    cy_send,
    cy_halo,
    cz_send,
    cz_halo,
    ratio,
    lap,
    weight,
    forcing,
    smooth,
    partial,
    sums,
    load_sem,
    dload_sem,
    send_sem,
    recv_sem,
    csend_sem,
    crecv_sem,
    rsend_sem,
    rrecv_sem,
):
    gx, gy, gz = sizes
    ix, iy, iz = lax.axis_index("gx"), lax.axis_index("gy"), lax.axis_index("gz")
    cheb = chebyshev(ITERS)

    across = (ix, iy, 1 - iz)
    targets = [
        (ix - 1, iy, iz),
        (ix + 1, iy, iz),
        (ix, iy - 1, iz),
        (ix, iy + 1, iz),
        across,
    ]
    exists = [ix > 0, ix < gx - 1, iy > 0, iy < gy - 1, None]
    order = (2, 3, 4, 0, 1)

    def where_exists(side):
        return (lambda f: f()) if exists[side] is None else pl.when(exists[side])

    counts = (8, 8, 4)
    places = (
        2 * lax.rem(ix, 4) + lax.rem(iy // 2, 2),
        4 * (ix // 4) + 2 * iz + lax.rem(iy, 2),
        iy // 4,
    )

    def peer(stage, o):
        other = lax.rem(places[stage] + o, counts[stage])
        return (
            (4 * (ix // 4) + other // 2, 4 * (iy // 4) + 2 * lax.rem(other, 2) + lax.rem(iy, 2), iz),
            (
                4 * (other // 4) + lax.rem(ix, 4),
                2 * (iy // 2) + lax.rem(other, 2),
                lax.rem(other // 2, 2),
            ),
            (ix, 4 * other + lax.rem(iy, 4), iz),
        )[stage]

    barrier = pltpu.get_barrier_semaphore()

    def greet(device):
        pl.semaphore_signal(barrier, inc=1, device_id=device, device_id_type=pl.DeviceIdType.MESH)

    for stage in GREETED:
        for o in range(1, counts[stage]):
            greet(peer(stage, o))
    for side in range(5):
        where_exists(side)(lambda: greet(targets[side]))
    greeted = 1 + sum(counts[stage] - 1 for stage in GREETED) + sum(jnp.where(here, 1, 0) for here in exists[:4])

    loads = [
        pltpu.make_async_copy(s_hbm, s_in, load_sem.at[0]),
        pltpu.make_async_copy(c_hbm, c_in, load_sem.at[1]),
        pltpu.make_async_copy(m_hbm, m_in, load_sem.at[2]),
    ]

    def load_group(g):
        dirs = pl.ds(g * PER, PER)
        return pltpu.make_async_copy(d_hbm.at[dirs], d_in.at[dirs], dload_sem.at[g])

    loads[0].start()
    for g in range(GROUPS):
        load_group(g).start()
    loads[1].start()
    loads[2].start()

    def faces(e, g):
        dirs = pl.ds(g * PER, PER)
        leave = [
            field.at[e, dirs, plane(0)],
            field.at[e, dirs, plane(EDGE - 1)],
            y_send.at[e, 0, dirs],
            y_send.at[e, 1, dirs],
            z_send.at[e, g],
        ]
        arrive = [
            field.at[e, dirs, plane(-1)],
            field.at[e, dirs, plane(EDGE)],
            y_halo.at[e, 0, dirs],
            y_halo.at[e, 1, dirs],
            z_halo.at[e, g],
        ]
        return leave, arrive, send_sem.at[e, g], recv_sem.at[e, g]

    def coef_faces(e):
        leave = [
            coef.at[e, plane(0)],
            coef.at[e, plane(EDGE - 1)],
            cy_send.at[e, 0],
            cy_send.at[e, 1],
            cz_send.at[e],
        ]
        arrive = [
            coef.at[e, plane(-1)],
            coef.at[e, plane(EDGE)],
            cy_halo.at[e, 0],
            cy_halo.at[e, 1],
            cz_halo.at[e],
        ]
        return leave, arrive, csend_sem.at[e], crecv_sem.at[e]

    opposite = (1, 0, 3, 2, 4)

    def outgoing(parts, side):
        leave, arrive, sent, received = parts
        return pltpu.make_async_remote_copy(
            src_ref=leave[side],
            dst_ref=arrive[opposite[side]],
            send_sem=sent.at[side],
            recv_sem=received.at[opposite[side]],
            device_id=targets[side],
            device_id_type=pl.DeviceIdType.MESH,
        )

    def incoming(parts, side):
        leave, arrive, sent, received = parts
        return pltpu.make_async_remote_copy(
            src_ref=leave[side],
            dst_ref=arrive[side],
            send_sem=sent.at[side],
            recv_sem=received.at[side],
            device_id=targets[side],
            device_id_type=pl.DeviceIdType.MESH,
        )

    def send(parts, sides=order):
        for side in sides:

            @where_exists(side)
            def _():
                outgoing(parts, side).start()

    def wait_faces(parts):
        for side in order:

            @where_exists(side)
            def _():
                incoming(parts, side).wait_recv()

    def wait_sent(parts):
        for side in order:

            @where_exists(side)
            def _():
                outgoing(parts, side).wait_send()

    nothing = jnp.zeros((EDGE, LANES), jnp.float32)
    for side in range(4):

        @pl.when(jnp.logical_not(exists[side]))
        def _():
            for e in range(2):
                if side < 2:
                    coef[e, plane(-1 if side == 0 else EDGE), :] = nothing
                else:
                    cy_halo[e, side - 2] = nothing

            @pl.loop(0, EXCHANGES)
            def _(e):
                for dd in range(NDIR):
                    if side < 2:
                        field[e, dd, plane(-1 if side == 0 else EDGE), :] = nothing
                    else:
                        y_halo[e, side - 2, dd] = nothing

    lane = lax.broadcasted_iota(jnp.int32, (EDGE, LANES), 1)
    first_lane, last_lane = lane == 0, lane == LANES - 1
    inner_lane = jnp.where(iz == 0, LANES - 1, 0)
    faces_partner = lane == inner_lane
    lane8 = lax.broadcasted_iota(jnp.int32, (8, LANES), 1)
    slot = lax.rem(lane8 - inner_lane + LANES, LANES)

    def pack(packed, values, place):
        for half in range(2):
            k = place + half
            moved = values[8 * half : 8 * half + 8]
            if k:
                moved = pltpu.roll(moved, k, 1)
            packed = jnp.where(slot == k, moved, packed)
        return packed

    def arrived(packed):
        return jnp.where(iz == 0, pltpu.roll(packed, LANES - 1, 1), pltpu.roll(packed, 1, 1))

    def unpack(packed, place):
        halves = [pltpu.roll(packed, (LANES - place - h) % LANES, 1) for h in range(2)]
        return jnp.concatenate(halves, axis=0)

    def stencil(load, x, packed, place):
        centre = load(0)
        below = jnp.where(first_lane, 0.0, pltpu.roll(centre, 1, 1))
        above = jnp.where(last_lane, 0.0, pltpu.roll(centre, LANES - 1, 1))
        beyond = jnp.where(faces_partner, unpack(packed, place), 0.0)
        total = (load(-PITCH) + load(PITCH)) + (load(-1) + load(1))
        return centre, total + ((below + above) + beyond)

    def field_stencil(e, dd, x, packed, dl):
        def load(offset):
            return field[e, dd, pl.ds((x + 1) * PITCH + offset, EDGE), :]

        return stencil(load, x, packed, dl * 2 * EDGE + 2 * x)

    empty = jnp.zeros((8, LANES), jnp.float32)

    def finish_coef(e, packed):
        cy_send[e, 0] = coef[e, row(0), :]
        cy_send[e, 1] = coef[e, row(EDGE - 1), :]
        cz_send[e] = packed
        send(coef_faces(e))

    def coef_rows(e):
        coef[e, row(-1), :] = cy_halo[e, 0]
        coef[e, row(EDGE), :] = cy_halo[e, 1]

    def finish_dir(e, dd):
        y_send[e, 0, dd] = field[e, dd, row(0), :]
        y_send[e, 1, dd] = field[e, dd, row(EDGE - 1), :]

    def field_rows(e, dd):
        field[e, dd, row(-1), :] = y_halo[e, 0, dd]
        field[e, dd, row(EDGE), :] = y_halo[e, 1, dd]

    loads[0].wait()
    packed = empty
    for x in range(EDGE):
        values = s_in[dense(x), :]
        coef[STATE, plane(x), :] = values
        packed = pack(packed, values, 2 * x)
    pl.semaphore_wait(barrier, greeted)
    finish_coef(STATE, packed)

    @pl.loop(0, GROUPS)
    def _(g):
        load_group(g).wait()
        packed = empty
        for dl in range(PER):
            dd = g * PER + dl
            for x in range(EDGE):
                values = d_in[dd, dense(x), :]
                field[DELTA, dd, plane(x), :] = values
                packed = pack(packed, values, dl * 2 * EDGE + 2 * x)
            finish_dir(DELTA, dd)
        z_send[DELTA, g] = packed
        send(faces(DELTA, g))

    loads[1].wait()
    for x in range(EDGE):
        conduct = jnp.exp(c_in[dense(x), :])
        ratio[dense(x), :] = conduct / (SHIFT + 6.0 * conduct)
    loads[2].wait()
    for x in range(EDGE):
        weight[dense(x), :] = DATA_WEIGHT * m_in[dense(x), :].astype(jnp.float32)

    wait_faces(coef_faces(STATE))
    coef_rows(STATE)
    state_z = arrived(cz_halo[STATE])
    packed = empty
    for x in range(EDGE):

        def load(offset, x=x):
            return coef[STATE, pl.ds((x + 1) * PITCH + offset, EDGE), :]

        centre, total = stencil(load, x, state_z, 2 * x)
        lap_here = 6.0 * centre - total
        lap[dense(x), :] = lap_here
        first = -cheb[0] * ratio[dense(x), :] * lap_here
        coef[FIRST, plane(x), :] = first
        packed = pack(packed, first, 2 * x)
    finish_coef(FIRST, packed)

    @pl.loop(0, GROUPS)
    def _(g):
        wait_faces(faces(DELTA, g))
        delta_z = arrived(z_halo[DELTA, g])
        for dl in range(PER):
            dd = g * PER + dl
            field_rows(DELTA, dd)
            total = nothing
            for x in range(EDGE):
                centre, near = field_stencil(DELTA, dd, x, delta_z, dl)
                part = BETA * (6.0 * centre - near)
                smooth[dd, dense(x), :] = part
                total = total + centre * part
                forcing[dd, dense(x), :] = -lap[dense(x), :] * centre
                field[T0, dd, plane(x), :] = coef[FIRST, plane(x), :] * centre
            partial[dd] = total[:8] + total[8:]

    def advance(g, src, packed, w, sink):
        for dl in range(PER):
            dd = g * PER + dl
            sink.begin()
            for x in range(EDGE):
                centre, near = field_stencil(src, dd, x, packed, dl)
                step = ratio[dense(x), :] * (forcing[dd, dense(x), :] + near) - centre
                sink.plane(dd, x, centre + w * step)
            sink.end(dd)
        sink.leave(g)

    class Iterate:
        def __init__(self, dst):
            self.dst = dst

        def begin(self):
            pass

        def plane(self, dd, x, values):
            field[self.dst, dd, plane(x), :] = values

        def end(self, dd):
            finish_dir(self.dst, dd)

        def leave(self, g):
            parts = faces(self.dst, g)
            send(parts, (2, 3, 0, 1))
            packed = empty
            for dl in range(PER):
                for x in range(EDGE):
                    values = field[self.dst, g * PER + dl, plane(x), :]
                    packed = pack(packed, values, dl * 2 * EDGE + 2 * x)
            z_send[self.dst, g] = packed
            send(parts, (4,))

    class Observe(Iterate):
        def begin(self):
            self.total = nothing

        def plane(self, dd, x, values):
            rhs = weight[dense(x), :] * values
            forcing[dd, dense(x), :] = rhs
            self.total = self.total + rhs * values
            super().plane(dd, x, cheb[0] * ratio[dense(x), :] * rhs)

        def end(self, dd):
            partial[dd] = partial[dd] + (self.total[:8] + self.total[8:])
            super().end(dd)

    class Result(Iterate):
        def __init__(self):
            pass

        def plane(self, dd, x, values):
            result[dd, dense(x), :] = smooth[dd, dense(x), :] - lap[dense(x), :] * values

        def end(self, dd):
            pass

        def leave(self, g):
            pass

    def step(src, sink, w):
        @pl.loop(0, GROUPS)
        def _(g):
            wait_faces(faces(src, g))
            for dl in range(PER):
                field_rows(src, g * PER + dl)
            advance(g, src, arrived(z_halo[src, g]), w, sink)

    wait_faces(coef_faces(FIRST))
    first_z = arrived(cz_halo[FIRST])
    repeated = first_z
    for dl in range(1, PER):
        repeated = repeated + pltpu.roll(first_z, dl * 2 * EDGE, 1)

    @pl.loop(0, GROUPS)
    def _(g):
        for dl in range(PER):
            dd = g * PER + dl
            for x in (-1, EDGE):
                field[T0, dd, plane(x), :] = coef[FIRST, plane(x), :] * field[DELTA, dd, plane(x), :]
            field[T0, dd, row(-1), :] = cy_halo[FIRST, 0] * y_halo[DELTA, 0, dd]
            field[T0, dd, row(EDGE), :] = cy_halo[FIRST, 1] * y_halo[DELTA, 1, dd]
        start_z = repeated * arrived(z_halo[DELTA, g])
        advance(g, T0, start_z, cheb[1], Iterate(T1))

    step(T1, Iterate(T2), cheb[2])
    step(T2, Observe(B0), cheb[3])

    def sum_copy(stage, place, o):
        return pltpu.make_async_remote_copy(
            src_ref=sums.at[stage, place],
            dst_ref=sums.at[stage, place],
            send_sem=rsend_sem.at[stage, o],
            recv_sem=rrecv_sem.at[stage, o],
            device_id=peer(stage, o),
            device_id_type=pl.DeviceIdType.MESH,
        )

    def sum_start(stage, value):
        sums[stage, places[stage]] = value
        for o in range(1, counts[stage]):
            sum_copy(stage, places[stage], o).start()

    def sum_end(stage):
        for o in range(1, counts[stage]):
            sum_copy(stage, lax.rem(places[stage] + counts[stage] - o, counts[stage]), o).wait_recv()
        parts = [sums[stage, place] for place in range(counts[stage])]
        while len(parts) > 1:
            parts = [p + q for p, q in zip(parts[::2], parts[1::2])]
        return parts[0]

    sum_start(0, jnp.sum(partial[...], axis=1))
    step(B0, Iterate(B1), cheb[1])
    sum_start(1, sum_end(0))
    step(B1, Iterate(B2), cheb[2])
    sum_start(2, sum_end(1))
    step(B2, Result(), cheb[3])
    quo_ref[...] = sum_end(2)

    @pl.loop(0, GROUPS)
    def _(g):
        for e in range(EXCHANGES):
            wait_sent(faces(e, g))

    for e in range(2):
        wait_sent(coef_faces(e))
    for stage in range(3):
        for o in range(1, counts[stage]):
            sum_copy(stage, places[stage], o).wait_send()


def finish(cells, sums, quo_ref):
    quo_ref[...] = jnp.sum(sums[...], axis=1) / cells


def solution(mesh):
    sizes = tuple(mesh.shape[name] for name in ("gx", "gy", "gz"))
    gx, gy, gz = sizes
    assert sizes == (8, 16, 2)
    f32 = jnp.float32
    cells = gx * gy * gz * DENSE * LANES

    def shards(directions, state, log_cond, obs_mask):
        assert directions.shape == (NDIR, EDGE, EDGE, LANES)
        any_spec = pl.BlockSpec(memory_space=pl.ANY)
        vmem_spec = pl.BlockSpec(memory_space=pltpu.VMEM)
        result, sums = pl.pallas_call(
            lambda *refs: kernel(sizes, *refs),
            out_shape=(
                pltpu.VMEM((NDIR, DENSE, LANES), f32),
                pltpu.VMEM((NDIR, LANES), f32),
            ),
            in_specs=[any_spec] * 4,
            out_specs=(vmem_spec, vmem_spec),
            scratch_shapes=[
                pltpu.VMEM((NDIR, DENSE, LANES), f32),
                pltpu.VMEM((DENSE, LANES), f32),
                pltpu.VMEM((DENSE, LANES), f32),
                pltpu.VMEM((DENSE, LANES), jnp.int32),
                pltpu.VMEM((EXCHANGES + 1, NDIR, ROWS, LANES), f32),
                pltpu.VMEM((EXCHANGES, 2, NDIR, EDGE, LANES), f32),
                pltpu.VMEM((EXCHANGES, 2, NDIR, EDGE, LANES), f32),
                pltpu.VMEM((EXCHANGES, GROUPS, 8, LANES), f32),
                pltpu.VMEM((EXCHANGES, GROUPS, 8, LANES), f32),
                pltpu.VMEM((2, ROWS, LANES), f32),
                pltpu.VMEM((2, 2, EDGE, LANES), f32),
                pltpu.VMEM((2, 2, EDGE, LANES), f32),
                pltpu.VMEM((2, 8, LANES), f32),
                pltpu.VMEM((2, 8, LANES), f32),
                pltpu.VMEM((DENSE, LANES), f32),
                pltpu.VMEM((DENSE, LANES), f32),
                pltpu.VMEM((DENSE, LANES), f32),
                pltpu.VMEM((NDIR, DENSE, LANES), f32),
                pltpu.VMEM((NDIR, DENSE, LANES), f32),
                pltpu.VMEM((NDIR, 8, LANES), f32),
                pltpu.VMEM((3, 8, NDIR, LANES), f32),
                pltpu.SemaphoreType.DMA((3,)),
                pltpu.SemaphoreType.DMA((GROUPS,)),
                pltpu.SemaphoreType.DMA((EXCHANGES, GROUPS, 5)),
                pltpu.SemaphoreType.DMA((EXCHANGES, GROUPS, 5)),
                pltpu.SemaphoreType.DMA((2, 5)),
                pltpu.SemaphoreType.DMA((2, 5)),
                pltpu.SemaphoreType.DMA((3, 8)),
                pltpu.SemaphoreType.DMA((3, 8)),
            ],
            compiler_params=pltpu.CompilerParams(collective_id=0, has_side_effects=True),
        )(
            directions.reshape(NDIR, DENSE, LANES),
            state.reshape(DENSE, LANES),
            log_cond.reshape(DENSE, LANES),
            obs_mask.reshape(DENSE, LANES),
        )
        quotient = pl.pallas_call(
            lambda *refs: finish(cells, *refs),
            out_shape=jax.ShapeDtypeStruct((NDIR,), f32),
            in_specs=[vmem_spec],
            out_specs=vmem_spec,
        )(pltpu.with_memory_space_constraint(sums, pltpu.VMEM))
        return result.reshape(directions.shape), quotient

    placed = P("gx", "gy", "gz")
    stacked = P(None, "gx", "gy", "gz")
    return jax.shard_map(
        shards,
        mesh=mesh,
        in_specs=(stacked, placed, placed, placed),
        out_specs=(stacked, P()),
        check_vma=False,
    )
```

```python
import math

import jax
import jax.numpy as jnp
from jax import lax
from jax.experimental import pallas as pl
from jax.experimental.pallas import tpu as pltpu
from jax.sharding import PartitionSpec as P

ITERS = 4
SHIFT = 0.3
BETA = 0.05
DATA_WEIGHT = 10.0

NDIR = 8
EDGE = 16
LANES = 128
DENSE = EDGE * EDGE
PITCH = 24
ROWS = (EDGE + 2) * PITCH
PER = 2
GROUPS = NDIR // PER

DELTA, T1, T2, B0, B1, B2, T0 = range(7)
EXCHANGES = 6
STATE, FIRST = range(2)
GREETED = (0, 1, 2)


def chebyshev(count):
    return [
        1.0 / (1.125 + 0.825 * math.cos(math.pi * (2 * j + 1) / (2 * count))) for j in range(count)
    ]


def dense(x):
    return pl.ds(x * EDGE, EDGE)


def plane(x):
    return pl.ds((x + 1) * PITCH, EDGE)


def row(y):
    return pl.ds(PITCH + y, EDGE, stride=PITCH)


def kernel(
    sizes,
    d_hbm,
    s_hbm,
    c_hbm,
    m_hbm,
    result,
    quo_ref,
    d_in,
    s_in,
    c_in,
    m_in,
    field,
    y_send,
    y_halo,
    z_send,
    z_halo,
    coef,
    cy_send,
    cy_halo,
    cz_send,
    cz_halo,
    ratio,
    lap,
    weight,
    forcing,
    smooth,
    partial,
    sums,
    load_sem,
    dload_sem,
    send_sem,
    recv_sem,
    csend_sem,
    crecv_sem,
    rsend_sem,
    rrecv_sem,
):
    gx, gy, gz = sizes
    ix, iy, iz = lax.axis_index("gx"), lax.axis_index("gy"), lax.axis_index("gz")
    cheb = chebyshev(ITERS)

    across = (ix, iy, 1 - iz)
    targets = [
        (ix - 1, iy, iz),
        (ix + 1, iy, iz),
        (ix, iy - 1, iz),
        (ix, iy + 1, iz),
        across,
    ]
    exists = [ix > 0, ix < gx - 1, iy > 0, iy < gy - 1, None]
    order = (2, 3, 4, 0, 1)

    def where_exists(side):
        return (lambda f: f()) if exists[side] is None else pl.when(exists[side])

    counts = (8, 4, 8)
    places = (
        2 * lax.rem(ix, 4) + lax.rem(iy // 2, 2),
        iy // 4,
        4 * (ix // 4) + 2 * iz + lax.rem(iy, 2),
    )

    def peer(stage, o):
        other = lax.rem(places[stage] + o, counts[stage])
        return (
            (4 * (ix // 4) + other // 2, 4 * (iy // 4) + 2 * lax.rem(other, 2) + lax.rem(iy, 2), iz),
            (ix, 4 * other + lax.rem(iy, 4), iz),
            (
                4 * (other // 4) + lax.rem(ix, 4),
                2 * (iy // 2) + lax.rem(other, 2),
                lax.rem(other // 2, 2),
            ),
        )[stage]

    loads = [
        pltpu.make_async_copy(s_hbm, s_in, load_sem.at[0]),
        pltpu.make_async_copy(c_hbm, c_in, load_sem.at[1]),
        pltpu.make_async_copy(m_hbm, m_in, load_sem.at[2]),
    ]

    def load_group(g):
        dirs = pl.ds(g * PER, PER)
        return pltpu.make_async_copy(d_hbm.at[dirs], d_in.at[dirs], dload_sem.at[g])

    loads[0].start()
    for g in range(GROUPS):
        load_group(g).start()
    loads[1].start()
    loads[2].start()

    barrier = pltpu.get_barrier_semaphore()

    def greet(device):
        pl.semaphore_signal(barrier, inc=1, device_id=device, device_id_type=pl.DeviceIdType.MESH)

    for stage in GREETED:
        for o in range(1, counts[stage]):
            greet(peer(stage, o))
    for side in range(5):
        where_exists(side)(lambda: greet(targets[side]))
    greeted = 1 + sum(counts[stage] - 1 for stage in GREETED) + sum(jnp.where(here, 1, 0) for here in exists[:4])

    def faces(e, g):
        dirs = pl.ds(g * PER, PER)
        leave = [
            field.at[e, dirs, plane(0)],
            field.at[e, dirs, plane(EDGE - 1)],
            y_send.at[e, 0, dirs],
            y_send.at[e, 1, dirs],
            z_send.at[e, g],
        ]
        arrive = [
            field.at[e, dirs, plane(-1)],
            field.at[e, dirs, plane(EDGE)],
            y_halo.at[e, 0, dirs],
            y_halo.at[e, 1, dirs],
            z_halo.at[e, g],
        ]
        return leave, arrive, send_sem.at[e, g], recv_sem.at[e, g]

    def coef_faces(e):
        leave = [
            coef.at[e, plane(0)],
            coef.at[e, plane(EDGE - 1)],
            cy_send.at[e, 0],
            cy_send.at[e, 1],
            cz_send.at[e],
        ]
        arrive = [
            coef.at[e, plane(-1)],
            coef.at[e, plane(EDGE)],
            cy_halo.at[e, 0],
            cy_halo.at[e, 1],
            cz_halo.at[e],
        ]
        return leave, arrive, csend_sem.at[e], crecv_sem.at[e]

    opposite = (1, 0, 3, 2, 4)

    def outgoing(parts, side):
        leave, arrive, sent, received = parts
        return pltpu.make_async_remote_copy(
            src_ref=leave[side],
            dst_ref=arrive[opposite[side]],
            send_sem=sent.at[side],
            recv_sem=received.at[opposite[side]],
            device_id=targets[side],
            device_id_type=pl.DeviceIdType.MESH,
        )

    def incoming(parts, side):
        leave, arrive, sent, received = parts
        return pltpu.make_async_remote_copy(
            src_ref=leave[side],
            dst_ref=arrive[side],
            send_sem=sent.at[side],
            recv_sem=received.at[side],
            device_id=targets[side],
            device_id_type=pl.DeviceIdType.MESH,
        )

    def send(parts, sides=order):
        for side in sides:

            @where_exists(side)
            def _():
                outgoing(parts, side).start()

    def wait_faces(parts):
        for side in order:

            @where_exists(side)
            def _():
                incoming(parts, side).wait_recv()

    def wait_sent(parts):
        for side in order:

            @where_exists(side)
            def _():
                outgoing(parts, side).wait_send()

    nothing = jnp.zeros((EDGE, LANES), jnp.float32)
    for side in range(4):

        @pl.when(jnp.logical_not(exists[side]))
        def _():
            for e in range(2):
                if side < 2:
                    coef[e, plane(-1 if side == 0 else EDGE), :] = nothing
                else:
                    cy_halo[e, side - 2] = nothing

            @pl.loop(0, EXCHANGES)
            def _(e):
                for dd in range(NDIR):
                    if side < 2:
                        field[e, dd, plane(-1 if side == 0 else EDGE), :] = nothing
                    else:
                        y_halo[e, side - 2, dd] = nothing

    lane = lax.broadcasted_iota(jnp.int32, (EDGE, LANES), 1)
    first_lane, last_lane = lane == 0, lane == LANES - 1
    inner_lane = jnp.where(iz == 0, LANES - 1, 0)
    faces_partner = lane == inner_lane
    lane8 = lax.broadcasted_iota(jnp.int32, (8, LANES), 1)
    slot = lax.rem(lane8 - inner_lane + LANES, LANES)

    def pack(packed, values, place):
        for half in range(2):
            k = place + half
            moved = values[8 * half : 8 * half + 8]
            if k:
                moved = pltpu.roll(moved, k, 1)
            packed = jnp.where(slot == k, moved, packed)
        return packed

    def arrived(packed):
        return jnp.where(iz == 0, pltpu.roll(packed, LANES - 1, 1), pltpu.roll(packed, 1, 1))

    def unpack(packed, place):
        halves = [pltpu.roll(packed, (LANES - place - h) % LANES, 1) for h in range(2)]
        return jnp.concatenate(halves, axis=0)

    def stencil(load, x, packed, place):
        centre = load(0)
        below = jnp.where(first_lane, 0.0, pltpu.roll(centre, 1, 1))
        above = jnp.where(last_lane, 0.0, pltpu.roll(centre, LANES - 1, 1))
        beyond = jnp.where(faces_partner, unpack(packed, place), 0.0)
        total = (load(-PITCH) + load(PITCH)) + (load(-1) + load(1))
        return centre, total + ((below + above) + beyond)

    def field_stencil(e, dd, x, packed, dl):
        def load(offset):
            return field[e, dd, pl.ds((x + 1) * PITCH + offset, EDGE), :]

        return stencil(load, x, packed, dl * 2 * EDGE + 2 * x)

    empty = jnp.zeros((8, LANES), jnp.float32)

    def finish_coef(e, packed):
        cy_send[e, 0] = coef[e, row(0), :]
        cy_send[e, 1] = coef[e, row(EDGE - 1), :]
        cz_send[e] = packed
        send(coef_faces(e))

    def coef_rows(e):
        coef[e, row(-1), :] = cy_halo[e, 0]
        coef[e, row(EDGE), :] = cy_halo[e, 1]

    def finish_dir(e, dd):
        y_send[e, 0, dd] = field[e, dd, row(0), :]
        y_send[e, 1, dd] = field[e, dd, row(EDGE - 1), :]

    def field_rows(e, dd):
        field[e, dd, row(-1), :] = y_halo[e, 0, dd]
        field[e, dd, row(EDGE), :] = y_halo[e, 1, dd]

    loads[0].wait()
    packed = empty
    for x in range(EDGE):
        values = s_in[dense(x), :]
        coef[STATE, plane(x), :] = values
        packed = pack(packed, values, 2 * x)
    pl.semaphore_wait(barrier, greeted)
    finish_coef(STATE, packed)

    @pl.loop(0, GROUPS)
    def _(g):
        load_group(g).wait()
        packed = empty
        for dl in range(PER):
            dd = g * PER + dl
            for x in range(EDGE):
                values = d_in[dd, dense(x), :]
                field[DELTA, dd, plane(x), :] = values
                packed = pack(packed, values, dl * 2 * EDGE + 2 * x)
            finish_dir(DELTA, dd)
        z_send[DELTA, g] = packed
        send(faces(DELTA, g))

    loads[1].wait()
    for x in range(EDGE):
        conduct = jnp.exp(c_in[dense(x), :])
        ratio[dense(x), :] = conduct / (SHIFT + 6.0 * conduct)
    loads[2].wait()
    for x in range(EDGE):
        weight[dense(x), :] = DATA_WEIGHT * m_in[dense(x), :].astype(jnp.float32)

    wait_faces(coef_faces(STATE))
    coef_rows(STATE)
    state_z = arrived(cz_halo[STATE])
    packed = empty
    for x in range(EDGE):

        def load(offset, x=x):
            return coef[STATE, pl.ds((x + 1) * PITCH + offset, EDGE), :]

        centre, total = stencil(load, x, state_z, 2 * x)
        lap_here = 6.0 * centre - total
        lap[dense(x), :] = lap_here
        first = -cheb[0] * ratio[dense(x), :] * lap_here
        coef[FIRST, plane(x), :] = first
        packed = pack(packed, first, 2 * x)
    finish_coef(FIRST, packed)

    @pl.loop(0, GROUPS)
    def _(g):
        wait_faces(faces(DELTA, g))
        delta_z = arrived(z_halo[DELTA, g])
        for dl in range(PER):
            dd = g * PER + dl
            field_rows(DELTA, dd)
            total = nothing
            for x in range(EDGE):
                centre, near = field_stencil(DELTA, dd, x, delta_z, dl)
                part = BETA * (6.0 * centre - near)
                smooth[dd, dense(x), :] = part
                total = total + centre * part
                forcing[dd, dense(x), :] = -lap[dense(x), :] * centre
                field[T0, dd, plane(x), :] = coef[FIRST, plane(x), :] * centre
            partial[dd] = total[:8] + total[8:]

    def sum_copy(stage, place, o):
        return pltpu.make_async_remote_copy(
            src_ref=sums.at[stage, place],
            dst_ref=sums.at[stage, place],
            send_sem=rsend_sem.at[stage, o],
            recv_sem=rrecv_sem.at[stage, o],
            device_id=peer(stage, o),
            device_id_type=pl.DeviceIdType.MESH,
        )

    def sum_start(stage, value):
        sums[stage, places[stage]] = value
        for o in range(1, counts[stage]):
            sum_copy(stage, places[stage], o).start()

    def sum_end(stage):
        for o in range(1, counts[stage]):
            sum_copy(stage, lax.rem(places[stage] + counts[stage] - o, counts[stage]), o).wait_recv()
        parts = [sums[stage, place] for place in range(counts[stage])]
        while len(parts) > 1:
            parts = [p + q for p, q in zip(parts[::2], parts[1::2])]
        return parts[0]

    def advance(g, src, packed, w, sink):
        for dl in range(PER):
            dd = g * PER + dl
            sink.begin()
            for x in range(EDGE):
                centre, near = field_stencil(src, dd, x, packed, dl)
                step = ratio[dense(x), :] * (forcing[dd, dense(x), :] + near) - centre
                sink.plane(dd, x, centre + w * step)
            sink.end(dd)
        sink.leave(g)

    class Iterate:
        def __init__(self, dst):
            self.dst = dst

        def begin(self):
            pass

        def plane(self, dd, x, values):
            field[self.dst, dd, plane(x), :] = values

        def end(self, dd):
            finish_dir(self.dst, dd)

        def leave(self, g):
            parts = faces(self.dst, g)
            send(parts, (2, 3, 0, 1))
            packed = empty
            for dl in range(PER):
                for x in range(EDGE):
                    values = field[self.dst, g * PER + dl, plane(x), :]
                    packed = pack(packed, values, dl * 2 * EDGE + 2 * x)
            z_send[self.dst, g] = packed
            send(parts, (4,))

    class Observe(Iterate):
        def begin(self):
            self.total = nothing

        def plane(self, dd, x, values):
            rhs = weight[dense(x), :] * values
            forcing[dd, dense(x), :] = rhs
            self.total = self.total + rhs * values
            super().plane(dd, x, cheb[0] * ratio[dense(x), :] * rhs)

        def end(self, dd):
            partial[dd] = partial[dd] + (self.total[:8] + self.total[8:])
            super().end(dd)

        def leave(self, g):
            @pl.when(g == GROUPS - 1)
            def _():
                sum_start(0, jnp.sum(partial[...], axis=1))

            super().leave(g)

    class Result(Iterate):
        def __init__(self):
            pass

        def plane(self, dd, x, values):
            result[dd, dense(x), :] = smooth[dd, dense(x), :] - lap[dense(x), :] * values

        def end(self, dd):
            pass

        def leave(self, g):
            pass

    def step(src, sink, w, after=None, then=None):
        @pl.loop(0, GROUPS)
        def _(g):
            wait_faces(faces(src, g))
            for dl in range(PER):
                field_rows(src, g * PER + dl)
            advance(g, src, arrived(z_halo[src, g]), w, sink)
            if then is not None:
                pl.when(g == after)(then)

    wait_faces(coef_faces(FIRST))
    first_z = arrived(cz_halo[FIRST])
    repeated = first_z
    for dl in range(1, PER):
        repeated = repeated + pltpu.roll(first_z, dl * 2 * EDGE, 1)

    @pl.loop(0, GROUPS)
    def _(g):
        for dl in range(PER):
            dd = g * PER + dl
            for x in (-1, EDGE):
                field[T0, dd, plane(x), :] = coef[FIRST, plane(x), :] * field[DELTA, dd, plane(x), :]
            field[T0, dd, row(-1), :] = cy_halo[FIRST, 0] * y_halo[DELTA, 0, dd]
            field[T0, dd, row(EDGE), :] = cy_halo[FIRST, 1] * y_halo[DELTA, 1, dd]
        start_z = repeated * arrived(z_halo[DELTA, g])
        advance(g, T0, start_z, cheb[1], Iterate(T1))

    step(T1, Iterate(T2), cheb[2])
    step(T2, Observe(B0), cheb[3])

    step(B0, Iterate(B1), cheb[1])
    sum_start(1, sum_end(0))
    step(B1, Iterate(B2), cheb[2])
    sum_start(2, sum_end(1))
    step(B2, Result(), cheb[3])
    quo_ref[...] = sum_end(2)

    @pl.loop(0, GROUPS)
    def _(g):
        for e in range(EXCHANGES):
            wait_sent(faces(e, g))

    for e in range(2):
        wait_sent(coef_faces(e))
    for stage in range(3):
        for o in range(1, counts[stage]):
            sum_copy(stage, places[stage], o).wait_send()


def finish(cells, result, sums, out_hbm, quo_ref, sem):
    parts = [pl.ds(d, 1) for d in range(NDIR)]
    copies = [pltpu.make_async_copy(result.at[p], out_hbm.at[p], sem.at[i]) for i, p in enumerate(parts)]
    for copy in copies:
        copy.start()
    quo_ref[...] = jnp.sum(sums[...], axis=1) / cells
    for copy in copies:
        copy.wait()


def solution(mesh):
    sizes = tuple(mesh.shape[name] for name in ("gx", "gy", "gz"))
    gx, gy, gz = sizes
    assert sizes == (8, 16, 2)
    f32 = jnp.float32
    cells = gx * gy * gz * DENSE * LANES

    def shards(directions, state, log_cond, obs_mask):
        assert directions.shape == (NDIR, EDGE, EDGE, LANES)
        any_spec = pl.BlockSpec(memory_space=pl.ANY)
        vmem_spec = pl.BlockSpec(memory_space=pltpu.VMEM)
        result, sums = pl.pallas_call(
            lambda *refs: kernel(sizes, *refs),
            out_shape=(
                pltpu.VMEM((NDIR, DENSE, LANES), f32),
                pltpu.VMEM((NDIR, LANES), f32),
            ),
            in_specs=[any_spec] * 4,
            out_specs=(vmem_spec, vmem_spec),
            scratch_shapes=[
                pltpu.VMEM((NDIR, DENSE, LANES), f32),
                pltpu.VMEM((DENSE, LANES), f32),
                pltpu.VMEM((DENSE, LANES), f32),
                pltpu.VMEM((DENSE, LANES), jnp.int32),
                pltpu.VMEM((EXCHANGES + 1, NDIR, ROWS, LANES), f32),
                pltpu.VMEM((EXCHANGES, 2, NDIR, EDGE, LANES), f32),
                pltpu.VMEM((EXCHANGES, 2, NDIR, EDGE, LANES), f32),
                pltpu.VMEM((EXCHANGES, GROUPS, 8, LANES), f32),
                pltpu.VMEM((EXCHANGES, GROUPS, 8, LANES), f32),
                pltpu.VMEM((2, ROWS, LANES), f32),
                pltpu.VMEM((2, 2, EDGE, LANES), f32),
                pltpu.VMEM((2, 2, EDGE, LANES), f32),
                pltpu.VMEM((2, 8, LANES), f32),
                pltpu.VMEM((2, 8, LANES), f32),
                pltpu.VMEM((DENSE, LANES), f32),
                pltpu.VMEM((DENSE, LANES), f32),
                pltpu.VMEM((DENSE, LANES), f32),
                pltpu.VMEM((NDIR, DENSE, LANES), f32),
                pltpu.VMEM((NDIR, DENSE, LANES), f32),
                pltpu.VMEM((NDIR, 8, LANES), f32),
                pltpu.VMEM((3, 8, NDIR, LANES), f32),
                pltpu.SemaphoreType.DMA((3,)),
                pltpu.SemaphoreType.DMA((GROUPS,)),
                pltpu.SemaphoreType.DMA((EXCHANGES, GROUPS, 5)),
                pltpu.SemaphoreType.DMA((EXCHANGES, GROUPS, 5)),
                pltpu.SemaphoreType.DMA((2, 5)),
                pltpu.SemaphoreType.DMA((2, 5)),
                pltpu.SemaphoreType.DMA((3, 8)),
                pltpu.SemaphoreType.DMA((3, 8)),
            ],
            compiler_params=pltpu.CompilerParams(collective_id=0, has_side_effects=True),
        )(
            directions.reshape(NDIR, DENSE, LANES),
            state.reshape(DENSE, LANES),
            log_cond.reshape(DENSE, LANES),
            obs_mask.reshape(DENSE, LANES),
        )
        result, sums = (pltpu.with_memory_space_constraint(v, pltpu.VMEM) for v in (result, sums))
        out, quotient = pl.pallas_call(
            lambda *refs: finish(cells, *refs),
            out_shape=(
                jax.ShapeDtypeStruct((NDIR, DENSE, LANES), f32),
                jax.ShapeDtypeStruct((NDIR,), f32),
            ),
            in_specs=[vmem_spec, vmem_spec],
            out_specs=(any_spec, vmem_spec),
            scratch_shapes=[pltpu.SemaphoreType.DMA((NDIR,))],
        )(result, sums)
        return out.reshape(directions.shape), quotient

    placed = P("gx", "gy", "gz")
    stacked = P(None, "gx", "gy", "gz")
    return jax.shard_map(
        shards,
        mesh=mesh,
        in_specs=(stacked, placed, placed, placed),
        out_specs=(stacked, P()),
        check_vma=False,
    )
```

```python
import math

import jax
import jax.numpy as jnp
from jax import lax
from jax.experimental import pallas as pl
from jax.experimental.pallas import tpu as pltpu
from jax.sharding import PartitionSpec as P

ITERS = 4
SHIFT = 0.3
BETA = 0.05
DATA_WEIGHT = 10.0

NDIR = 8
EDGE = 16
LANES = 128
DENSE = EDGE * EDGE
PITCH = 24
ROWS = (EDGE + 2) * PITCH
PER = 2
GROUPS = NDIR // PER

DELTA, T1, T2, B0, B1, B2, T0 = range(7)
EXCHANGES = 6
STATE, FIRST = range(2)
GREETED = (1,)


def chebyshev(count):
    return [
        1.0 / (1.125 + 0.825 * math.cos(math.pi * (2 * j + 1) / (2 * count))) for j in range(count)
    ]


def dense(x):
    return pl.ds(x * EDGE, EDGE)


def plane(x):
    return pl.ds((x + 1) * PITCH, EDGE)


def row(y):
    return pl.ds(PITCH + y, EDGE, stride=PITCH)


def kernel(
    sizes,
    d_hbm,
    s_hbm,
    c_hbm,
    m_hbm,
    result,
    quo_ref,
    d_in,
    s_in,
    c_in,
    m_in,
    field,
    y_send,
    y_halo,
    z_send,
    z_halo,
    coef,
    cy_send,
    cy_halo,
    cz_send,
    cz_halo,
    ratio,
    lap,
    weight,
    forcing,
    smooth,
    partial,
    sums,
    load_sem,
    dload_sem,
    send_sem,
    recv_sem,
    csend_sem,
    crecv_sem,
    rsend_sem,
    rrecv_sem,
):
    gx, gy, gz = sizes
    ix, iy, iz = lax.axis_index("gx"), lax.axis_index("gy"), lax.axis_index("gz")
    cheb = chebyshev(ITERS)

    across = (ix, iy, 1 - iz)
    targets = [
        (ix - 1, iy, iz),
        (ix + 1, iy, iz),
        (ix, iy - 1, iz),
        (ix, iy + 1, iz),
        across,
    ]
    exists = [ix > 0, ix < gx - 1, iy > 0, iy < gy - 1, None]
    order = (2, 3, 4, 0, 1)

    def where_exists(side):
        return (lambda f: f()) if exists[side] is None else pl.when(exists[side])

    counts = (8, 4, 8)
    places = (
        2 * lax.rem(ix, 4) + lax.rem(iy // 2, 2),
        iy // 4,
        4 * (ix // 4) + 2 * iz + lax.rem(iy, 2),
    )

    def peer(stage, o):
        other = lax.rem(places[stage] + o, counts[stage])
        return (
            (4 * (ix // 4) + other // 2, 4 * (iy // 4) + 2 * lax.rem(other, 2) + lax.rem(iy, 2), iz),
            (ix, 4 * other + lax.rem(iy, 4), iz),
            (
                4 * (other // 4) + lax.rem(ix, 4),
                2 * (iy // 2) + lax.rem(other, 2),
                lax.rem(other // 2, 2),
            ),
        )[stage]

    loads = [
        pltpu.make_async_copy(s_hbm, s_in, load_sem.at[0]),
        pltpu.make_async_copy(c_hbm, c_in, load_sem.at[1]),
        pltpu.make_async_copy(m_hbm, m_in, load_sem.at[2]),
    ]

    def load_group(g):
        dirs = pl.ds(g * PER, PER)
        return pltpu.make_async_copy(d_hbm.at[dirs], d_in.at[dirs], dload_sem.at[g])

    loads[0].start()
    for g in range(GROUPS):
        load_group(g).start()
    loads[1].start()
    loads[2].start()

    barrier = pltpu.get_barrier_semaphore()

    def greet(device):
        pl.semaphore_signal(barrier, inc=1, device_id=device, device_id_type=pl.DeviceIdType.MESH)

    for stage in GREETED:
        for o in range(1, counts[stage]):
            greet(peer(stage, o))
    for side in range(5):
        where_exists(side)(lambda: greet(targets[side]))
    greeted = 1 + sum(counts[stage] - 1 for stage in GREETED) + sum(jnp.where(here, 1, 0) for here in exists[:4])

    def faces(e, g):
        dirs = pl.ds(g * PER, PER)
        leave = [
            field.at[e, dirs, plane(0)],
            field.at[e, dirs, plane(EDGE - 1)],
            y_send.at[e, 0, dirs],
            y_send.at[e, 1, dirs],
            z_send.at[e, g],
        ]
        arrive = [
            field.at[e, dirs, plane(-1)],
            field.at[e, dirs, plane(EDGE)],
            y_halo.at[e, 0, dirs],
            y_halo.at[e, 1, dirs],
            z_halo.at[e, g],
        ]
        return leave, arrive, send_sem.at[e, g], recv_sem.at[e, g]

    def coef_faces(e):
        leave = [
            coef.at[e, plane(0)],
            coef.at[e, plane(EDGE - 1)],
            cy_send.at[e, 0],
            cy_send.at[e, 1],
            cz_send.at[e],
        ]
        arrive = [
            coef.at[e, plane(-1)],
            coef.at[e, plane(EDGE)],
            cy_halo.at[e, 0],
            cy_halo.at[e, 1],
            cz_halo.at[e],
        ]
        return leave, arrive, csend_sem.at[e], crecv_sem.at[e]

    opposite = (1, 0, 3, 2, 4)

    def outgoing(parts, side):
        leave, arrive, sent, received = parts
        return pltpu.make_async_remote_copy(
            src_ref=leave[side],
            dst_ref=arrive[opposite[side]],
            send_sem=sent.at[side],
            recv_sem=received.at[opposite[side]],
            device_id=targets[side],
            device_id_type=pl.DeviceIdType.MESH,
        )

    def incoming(parts, side):
        leave, arrive, sent, received = parts
        return pltpu.make_async_remote_copy(
            src_ref=leave[side],
            dst_ref=arrive[side],
            send_sem=sent.at[side],
            recv_sem=received.at[side],
            device_id=targets[side],
            device_id_type=pl.DeviceIdType.MESH,
        )

    def send(parts, sides=order):
        for side in sides:

            @where_exists(side)
            def _():
                outgoing(parts, side).start()

    def wait_faces(parts):
        for side in order:

            @where_exists(side)
            def _():
                incoming(parts, side).wait_recv()

    def wait_sent(parts):
        for side in order:

            @where_exists(side)
            def _():
                outgoing(parts, side).wait_send()

    nothing = jnp.zeros((EDGE, LANES), jnp.float32)
    for side in range(4):

        @pl.when(jnp.logical_not(exists[side]))
        def _():
            for e in range(2):
                if side < 2:
                    coef[e, plane(-1 if side == 0 else EDGE), :] = nothing
                else:
                    cy_halo[e, side - 2] = nothing

            @pl.loop(0, EXCHANGES)
            def _(e):
                for dd in range(NDIR):
                    if side < 2:
                        field[e, dd, plane(-1 if side == 0 else EDGE), :] = nothing
                    else:
                        y_halo[e, side - 2, dd] = nothing

    lane = lax.broadcasted_iota(jnp.int32, (EDGE, LANES), 1)
    first_lane, last_lane = lane == 0, lane == LANES - 1
    inner_lane = jnp.where(iz == 0, LANES - 1, 0)
    faces_partner = lane == inner_lane
    lane8 = lax.broadcasted_iota(jnp.int32, (8, LANES), 1)
    slot = lax.rem(lane8 - inner_lane + LANES, LANES)

    def pack(packed, values, place):
        for half in range(2):
            k = place + half
            moved = values[8 * half : 8 * half + 8]
            if k:
                moved = pltpu.roll(moved, k, 1)
            packed = jnp.where(slot == k, moved, packed)
        return packed

    def arrived(packed):
        return jnp.where(iz == 0, pltpu.roll(packed, LANES - 1, 1), pltpu.roll(packed, 1, 1))

    def unpack(packed, place):
        halves = [pltpu.roll(packed, (LANES - place - h) % LANES, 1) for h in range(2)]
        return jnp.concatenate(halves, axis=0)

    def stencil(load, x, packed, place):
        centre = load(0)
        below = jnp.where(first_lane, 0.0, pltpu.roll(centre, 1, 1))
        above = jnp.where(last_lane, 0.0, pltpu.roll(centre, LANES - 1, 1))
        beyond = jnp.where(faces_partner, unpack(packed, place), 0.0)
        total = (load(-PITCH) + load(PITCH)) + (load(-1) + load(1))
        return centre, total + ((below + above) + beyond)

    def field_stencil(e, dd, x, packed, dl):
        def load(offset):
            return field[e, dd, pl.ds((x + 1) * PITCH + offset, EDGE), :]

        return stencil(load, x, packed, dl * 2 * EDGE + 2 * x)

    empty = jnp.zeros((8, LANES), jnp.float32)

    def finish_coef(e, packed):
        cy_send[e, 0] = coef[e, row(0), :]
        cy_send[e, 1] = coef[e, row(EDGE - 1), :]
        cz_send[e] = packed
        send(coef_faces(e))

    def coef_rows(e):
        coef[e, row(-1), :] = cy_halo[e, 0]
        coef[e, row(EDGE), :] = cy_halo[e, 1]

    def finish_dir(e, dd):
        y_send[e, 0, dd] = field[e, dd, row(0), :]
        y_send[e, 1, dd] = field[e, dd, row(EDGE - 1), :]

    def field_rows(e, dd):
        field[e, dd, row(-1), :] = y_halo[e, 0, dd]
        field[e, dd, row(EDGE), :] = y_halo[e, 1, dd]

    loads[0].wait()
    packed = empty
    for x in range(EDGE):
        values = s_in[dense(x), :]
        coef[STATE, plane(x), :] = values
        packed = pack(packed, values, 2 * x)
    pl.semaphore_wait(barrier, greeted)
    finish_coef(STATE, packed)

    @pl.loop(0, GROUPS)
    def _(g):
        load_group(g).wait()
        packed = empty
        for dl in range(PER):
            dd = g * PER + dl
            for x in range(EDGE):
                values = d_in[dd, dense(x), :]
                field[DELTA, dd, plane(x), :] = values
                packed = pack(packed, values, dl * 2 * EDGE + 2 * x)
            finish_dir(DELTA, dd)
        z_send[DELTA, g] = packed
        send(faces(DELTA, g))

    loads[1].wait()
    for x in range(EDGE):
        conduct = jnp.exp(c_in[dense(x), :])
        ratio[dense(x), :] = conduct / (SHIFT + 6.0 * conduct)
    loads[2].wait()
    for x in range(EDGE):
        weight[dense(x), :] = DATA_WEIGHT * m_in[dense(x), :].astype(jnp.float32)

    wait_faces(coef_faces(STATE))
    coef_rows(STATE)
    state_z = arrived(cz_halo[STATE])
    packed = empty
    for x in range(EDGE):

        def load(offset, x=x):
            return coef[STATE, pl.ds((x + 1) * PITCH + offset, EDGE), :]

        centre, total = stencil(load, x, state_z, 2 * x)
        lap_here = 6.0 * centre - total
        lap[dense(x), :] = lap_here
        first = -cheb[0] * ratio[dense(x), :] * lap_here
        coef[FIRST, plane(x), :] = first
        packed = pack(packed, first, 2 * x)
    finish_coef(FIRST, packed)

    @pl.loop(0, GROUPS)
    def _(g):
        wait_faces(faces(DELTA, g))
        delta_z = arrived(z_halo[DELTA, g])
        for dl in range(PER):
            dd = g * PER + dl
            field_rows(DELTA, dd)
            total = nothing
            for x in range(EDGE):
                centre, near = field_stencil(DELTA, dd, x, delta_z, dl)
                part = BETA * (6.0 * centre - near)
                smooth[dd, dense(x), :] = part
                total = total + centre * part
                forcing[dd, dense(x), :] = -lap[dense(x), :] * centre
                field[T0, dd, plane(x), :] = coef[FIRST, plane(x), :] * centre
            partial[dd] = total[:8] + total[8:]

    def sum_copy(stage, place, o):
        return pltpu.make_async_remote_copy(
            src_ref=sums.at[stage, place],
            dst_ref=sums.at[stage, place],
            send_sem=rsend_sem.at[stage, o],
            recv_sem=rrecv_sem.at[stage, o],
            device_id=peer(stage, o),
            device_id_type=pl.DeviceIdType.MESH,
        )

    def sum_start(stage, value):
        sums[stage, places[stage]] = value
        for o in range(1, counts[stage]):
            sum_copy(stage, places[stage], o).start()

    def sum_end(stage):
        for o in range(1, counts[stage]):
            sum_copy(stage, lax.rem(places[stage] + counts[stage] - o, counts[stage]), o).wait_recv()
        parts = [sums[stage, place] for place in range(counts[stage])]
        while len(parts) > 1:
            parts = [p + q for p, q in zip(parts[::2], parts[1::2])]
        return parts[0]

    def advance(g, src, packed, w, sink):
        for dl in range(PER):
            dd = g * PER + dl
            sink.begin()
            for x in range(EDGE):
                centre, near = field_stencil(src, dd, x, packed, dl)
                step = ratio[dense(x), :] * (forcing[dd, dense(x), :] + near) - centre
                sink.plane(dd, x, centre + w * step)
            sink.end(dd)
        sink.leave(g)

    class Iterate:
        def __init__(self, dst):
            self.dst = dst

        def begin(self):
            pass

        def plane(self, dd, x, values):
            field[self.dst, dd, plane(x), :] = values

        def end(self, dd):
            finish_dir(self.dst, dd)

        def leave(self, g):
            parts = faces(self.dst, g)
            send(parts, (2, 3, 0, 1))
            packed = empty
            for dl in range(PER):
                for x in range(EDGE):
                    values = field[self.dst, g * PER + dl, plane(x), :]
                    packed = pack(packed, values, dl * 2 * EDGE + 2 * x)
            z_send[self.dst, g] = packed
            send(parts, (4,))

    class Observe(Iterate):
        def begin(self):
            self.total = nothing

        def plane(self, dd, x, values):
            rhs = weight[dense(x), :] * values
            forcing[dd, dense(x), :] = rhs
            self.total = self.total + rhs * values
            super().plane(dd, x, cheb[0] * ratio[dense(x), :] * rhs)

        def end(self, dd):
            partial[dd] = partial[dd] + (self.total[:8] + self.total[8:])
            super().end(dd)

        def leave(self, g):
            @pl.when(g == GROUPS - 1)
            def _():
                sum_start(0, jnp.sum(partial[...], axis=1))

            super().leave(g)

    class Result(Iterate):
        def __init__(self):
            pass

        def plane(self, dd, x, values):
            result[dd, dense(x), :] = smooth[dd, dense(x), :] - lap[dense(x), :] * values

        def end(self, dd):
            pass

        def leave(self, g):
            pass

    def step(src, sink, w, after=None, then=None):
        @pl.loop(0, GROUPS)
        def _(g):
            wait_faces(faces(src, g))
            for dl in range(PER):
                field_rows(src, g * PER + dl)
            advance(g, src, arrived(z_halo[src, g]), w, sink)
            if then is not None:
                pl.when(g == after)(then)

    wait_faces(coef_faces(FIRST))
    first_z = arrived(cz_halo[FIRST])
    repeated = first_z
    for dl in range(1, PER):
        repeated = repeated + pltpu.roll(first_z, dl * 2 * EDGE, 1)

    @pl.loop(0, GROUPS)
    def _(g):
        for dl in range(PER):
            dd = g * PER + dl
            for x in (-1, EDGE):
                field[T0, dd, plane(x), :] = coef[FIRST, plane(x), :] * field[DELTA, dd, plane(x), :]
            field[T0, dd, row(-1), :] = cy_halo[FIRST, 0] * y_halo[DELTA, 0, dd]
            field[T0, dd, row(EDGE), :] = cy_halo[FIRST, 1] * y_halo[DELTA, 1, dd]
        start_z = repeated * arrived(z_halo[DELTA, g])
        advance(g, T0, start_z, cheb[1], Iterate(T1))

    step(T1, Iterate(T2), cheb[2])
    step(T2, Observe(B0), cheb[3])

    step(B0, Iterate(B1), cheb[1])
    sum_start(1, sum_end(0))
    step(B1, Iterate(B2), cheb[2])
    sum_start(2, sum_end(1))
    step(B2, Result(), cheb[3])
    quo_ref[...] = sum_end(2)

    @pl.loop(0, GROUPS)
    def _(g):
        for e in range(EXCHANGES):
            wait_sent(faces(e, g))

    for e in range(2):
        wait_sent(coef_faces(e))
    for stage in range(3):
        for o in range(1, counts[stage]):
            sum_copy(stage, places[stage], o).wait_send()


def finish(cells, result, sums, out_hbm, quo_ref, sem):
    parts = [pl.ds(d, 1) for d in range(NDIR)]
    copies = [pltpu.make_async_copy(result.at[p], out_hbm.at[p], sem.at[i]) for i, p in enumerate(parts)]
    for copy in copies:
        copy.start()
    quo_ref[...] = jnp.sum(sums[...], axis=1) / cells
    for copy in copies:
        copy.wait()


def solution(mesh):
    sizes = tuple(mesh.shape[name] for name in ("gx", "gy", "gz"))
    gx, gy, gz = sizes
    assert sizes == (8, 16, 2)
    f32 = jnp.float32
    cells = gx * gy * gz * DENSE * LANES

    def shards(directions, state, log_cond, obs_mask):
        assert directions.shape == (NDIR, EDGE, EDGE, LANES)
        any_spec = pl.BlockSpec(memory_space=pl.ANY)
        vmem_spec = pl.BlockSpec(memory_space=pltpu.VMEM)
        result, sums = pl.pallas_call(
            lambda *refs: kernel(sizes, *refs),
            out_shape=(
                pltpu.VMEM((NDIR, DENSE, LANES), f32),
                pltpu.VMEM((NDIR, LANES), f32),
            ),
            in_specs=[any_spec] * 4,
            out_specs=(vmem_spec, vmem_spec),
            scratch_shapes=[
                pltpu.VMEM((NDIR, DENSE, LANES), f32),
                pltpu.VMEM((DENSE, LANES), f32),
                pltpu.VMEM((DENSE, LANES), f32),
                pltpu.VMEM((DENSE, LANES), jnp.int32),
                pltpu.VMEM((EXCHANGES + 1, NDIR, ROWS, LANES), f32),
                pltpu.VMEM((EXCHANGES, 2, NDIR, EDGE, LANES), f32),
                pltpu.VMEM((EXCHANGES, 2, NDIR, EDGE, LANES), f32),
                pltpu.VMEM((EXCHANGES, GROUPS, 8, LANES), f32),
                pltpu.VMEM((EXCHANGES, GROUPS, 8, LANES), f32),
                pltpu.VMEM((2, ROWS, LANES), f32),
                pltpu.VMEM((2, 2, EDGE, LANES), f32),
                pltpu.VMEM((2, 2, EDGE, LANES), f32),
                pltpu.VMEM((2, 8, LANES), f32),
                pltpu.VMEM((2, 8, LANES), f32),
                pltpu.VMEM((DENSE, LANES), f32),
                pltpu.VMEM((DENSE, LANES), f32),
                pltpu.VMEM((DENSE, LANES), f32),
                pltpu.VMEM((NDIR, DENSE, LANES), f32),
                pltpu.VMEM((NDIR, DENSE, LANES), f32),
                pltpu.VMEM((NDIR, 8, LANES), f32),
                pltpu.VMEM((3, 8, NDIR, LANES), f32),
                pltpu.SemaphoreType.DMA((3,)),
                pltpu.SemaphoreType.DMA((GROUPS,)),
                pltpu.SemaphoreType.DMA((EXCHANGES, GROUPS, 5)),
                pltpu.SemaphoreType.DMA((EXCHANGES, GROUPS, 5)),
                pltpu.SemaphoreType.DMA((2, 5)),
                pltpu.SemaphoreType.DMA((2, 5)),
                pltpu.SemaphoreType.DMA((3, 8)),
                pltpu.SemaphoreType.DMA((3, 8)),
            ],
            compiler_params=pltpu.CompilerParams(collective_id=0, has_side_effects=True),
        )(
            directions.reshape(NDIR, DENSE, LANES),
            state.reshape(DENSE, LANES),
            log_cond.reshape(DENSE, LANES),
            obs_mask.reshape(DENSE, LANES),
        )
        result, sums = (pltpu.with_memory_space_constraint(v, pltpu.VMEM) for v in (result, sums))
        out, quotient = pl.pallas_call(
            lambda *refs: finish(cells, *refs),
            out_shape=(
                jax.ShapeDtypeStruct((NDIR, DENSE, LANES), f32),
                jax.ShapeDtypeStruct((NDIR,), f32),
            ),
            in_specs=[vmem_spec, vmem_spec],
            out_specs=(any_spec, vmem_spec),
            scratch_shapes=[pltpu.SemaphoreType.DMA((NDIR,))],
        )(result, sums)
        return out.reshape(directions.shape), quotient

    placed = P("gx", "gy", "gz")
    stacked = P(None, "gx", "gy", "gz")
    return jax.shard_map(
        shards,
        mesh=mesh,
        in_specs=(stacked, placed, placed, placed),
        out_specs=(stacked, P()),
        check_vma=False,
    )
```
